32 devices in a mesh: row: 8 (over z, core), col: 4 (over y, x).
Axes of the slice: x: 2, y: 2, z: 4, core: 2. Of those that a mesh axis runs over, the one named last changes fastest.
Arguments:
- reference_image: float32 [1024, 1024], P('row', 'col'), may hold values from -6 to 6
- source_images: float32 [4, 1024, 1024], P(None, 'row', 'col'), may hold values from -6 to 6
- hypotheses: int32 [8, 1024, 1024], P(None, 'row', 'col'), may hold values from 0 to 15
- source_ids: int32 [4], replicated, may hold values from 1 to 3
- coarse_disp: float32 [128, 128], P('col'), may hold values from 0 to 15
- coarse_conf: float32 [128, 128], P('col'), may hold values from 0.1 to 10
Outputs:
- disparity: float32 [1024, 1024], P('row', 'col')
The draws below stay inside these ranges and needn't reach their ends.
All inputs are finite; a program needn't handle non-finite values.
Results may differ from the reference program's by a relative error of at most 0.0003.
Values sent between devices are 32-bit elements; how exact they have to be, the bound alone decides.
A program may use at most 64 MiB of HBM per device.

```python
import math
import jax
import jax.numpy as jnp
from jax import lax

LEVELS = 16
HYP = 8
SRC = 4
MAXID = 3
WIN = 11
UPS = 8
CITER = 4
H = 1024
W = 1024
CH = 128
CW = 128


def plant(array, own_key, smallest, top_value):
    shape = array.shape
    spot = [jax.random.randint(jax.random.fold_in(own_key, axis), (), 0, shape[axis]) for axis in range(len(shape))]
    array = array.at[tuple(spot)].set(smallest)
    longest = shape.index(max(shape))
    spot[longest] = (spot[longest] + 1) % shape[longest]
    return array.at[tuple(spot)].set(top_value)


def levels(key, dims, cuts, low, high):
    factor_of, own = 1.0, jax.random.fold_in(key, 6)
    for position, shards_of in cuts:
        steps = jnp.exp(jax.random.uniform(jax.random.fold_in(own, position), (shards_of,), jnp.float32, low / len(cuts), high / len(cuts)))
        factor_of = factor_of * jnp.repeat(steps, dims[position] // shards_of).reshape([-1 if axis == position else 1 for axis in range(len(dims))])
    return factor_of


def bell_draw(stream_key, shape, scale, bound, pieces=(), held_as=jnp.bfloat16):
    values = scale * jax.random.normal(stream_key, shape, jnp.float32)
    if pieces:
        values = values * levels(stream_key, shape, pieces, -0.22, 0.18)
    return jnp.clip(values, -bound, bound).astype(held_as)


def setup_inputs(seed: int = 0) -> dict:
    keys = jax.random.split(jax.random.key(seed), 7)
    return {
        "reference_image": bell_draw(keys[0], (H, W), 1.0, 6.0, ((0, 8), (1, 4)), jnp.float32),
        "source_images": bell_draw(keys[1], (SRC, H, W), 1.0, 6.0, ((1, 8), (2, 4)), jnp.float32),
        "hypotheses": plant(jax.random.randint(keys[2], (HYP, H, W), 0, LEVELS), jax.random.fold_in(keys[2], 1), 0, LEVELS - 1).astype(jnp.int32),
        "source_ids": plant(jax.random.randint(keys[3], (SRC,), 1, MAXID + 1), jax.random.fold_in(keys[3], 1), 1, MAXID).astype(jnp.int32),
        "coarse_disp": jnp.clip(15.0 * jax.random.uniform(keys[4], (CH, CW), jnp.float32) ** levels(keys[4], (CH, CW), ((0, 4),), -0.2, 0.2), 0.0, 15.0),
        "coarse_conf": jnp.clip(jnp.exp(math.log(10.0) - 4.6051702 * jax.random.uniform(keys[5], (CH, CW), jnp.float32) ** levels(keys[5], (CH, CW), ((0, 4),), -0.2, 0.2)), 0.1, 10.0),
    }


smooth_pull = 1.0
previous_estimate_factor = 0.01
exponential_sharpness = 0.1
variance_floor = 1e-05

def window_sums(values):
    radius = WIN // 2
    widths = [(0, 0)] * (values.ndim - 2) + [(radius, radius), (radius, radius)]
    padded = jnp.pad(values, widths)
    height = values.shape[-2]
    width_cols = values.shape[-1]
    row_sums = padded[..., 0:height, :]
    for offset in range(1, WIN):
        row_sums = row_sums + padded[..., offset:offset + height, :]
    accumulated_sums = row_sums[..., 0:width_cols]
    for offset in range(1, WIN):
        accumulated_sums = accumulated_sums + row_sums[..., offset:offset + width_cols]
    return accumulated_sums

def interp_matrix(fine_start, fine_count, coarse_start, coarse_pixel_number, coarse_total):
    fine_pos = fine_start + jnp.arange(fine_count, dtype=jnp.int32)
    numerator = 2 * fine_pos + 1 - UPS
    lower = numerator // (2 * UPS)
    fraction = (numerator - lower * 2 * UPS).astype(jnp.float32) / (2.0 * UPS)
    low_index = jnp.clip(lower, 0, coarse_total - 1) - coarse_start
    high_index = jnp.clip(lower + 1, 0, coarse_total - 1) - coarse_start
    columns = jnp.arange(coarse_pixel_number, dtype=jnp.int32)
    low_part = jnp.where(columns[None, :] == low_index[:, None], 1.0 - fraction[:, None], 0.0)
    high_part = jnp.where(columns[None, :] == high_index[:, None], fraction[:, None], 0.0)
    return low_part + high_part

def jacobi_step(padded_line_span, disp, conf):
    middle = padded_line_span[1:-1]
    col_pad = jnp.pad(middle, ((0, 0), (1, 1)))
    neighbours = padded_line_span[:-2] + padded_line_span[2:] + col_pad[:, :-2] + col_pad[:, 2:]
    return (conf * disp + smooth_pull * neighbours) / (conf + 4.0 * smooth_pull)

def estimate(chosen_hypothesis, candidate, centre):
    neighbour_jump_cost = 1.0 - chosen_hypothesis + previous_estimate_factor * (candidate - centre[None]) ** 2
    candidate_mixing_shares = jnp.exp(-neighbour_jump_cost / exponential_sharpness)
    return lax.optimization_barrier(jnp.sum(candidate_mixing_shares * candidate, axis=0)) / lax.optimization_barrier(jnp.sum(candidate_mixing_shares, axis=0))

def reference(reference_image, source_images, hypotheses, source_ids, coarse_disp, coarse_conf):
    current = coarse_disp
    for sweep in range(CITER):
        current = jacobi_step(jnp.pad(current, ((1, 1), (0, 0))), coarse_disp, coarse_conf)
    rows_mat = interp_matrix(0, H, 0, CH, CH)
    cols_mat = interp_matrix(0, W, 0, CW, CW)
    upsampled = jnp.dot(jnp.dot(rows_mat, current, precision=lax.Precision.HIGHEST), cols_mat.T, precision=lax.Precision.HIGHEST)
    area = float(WIN * WIN)
    shift_most = MAXID * (LEVELS - 1)
    wide = jnp.pad(source_images, ((0, 0), (0, 0), (shift_most, 0)))
    src_mean = window_sums(wide) / area
    src_var = window_sums(wide * wide) / area - src_mean ** 2 + variance_floor
    ref_mean = window_sums(reference_image) / area
    ref_var = window_sums(reference_image * reference_image) / area - ref_mean ** 2 + variance_floor

    def level_step(chosen_hypothesis, depth_level):
        ncc_sum = jnp.zeros((H, W), jnp.float32)
        for view_slot in range(SRC):
            begin_col = (shift_most - source_ids[view_slot] * depth_level).astype(jnp.int32)
            shifted = lax.dynamic_slice_in_dim(wide[view_slot], begin_col, W, 1)
            cross = window_sums(reference_image * shifted) / area
            mean_src = lax.dynamic_slice_in_dim(src_mean[view_slot], begin_col, W, 1)
            var_src = lax.dynamic_slice_in_dim(src_var[view_slot], begin_col, W, 1)
            ncc_sum = ncc_sum + (cross - ref_mean * mean_src) / jnp.sqrt(ref_var * var_src)
        volume = ncc_sum / SRC
        return (chosen_hypothesis + jnp.where(hypotheses == depth_level, volume[None], 0.0), None)
    chosen_hypothesis, unused = lax.scan(level_step, jnp.zeros((HYP, H, W), jnp.float32), jnp.arange(LEVELS, dtype=jnp.int32))
    candidate = hypotheses.astype(jnp.float32)
    red = estimate(chosen_hypothesis, candidate, upsampled)
    padded_red = jnp.pad(red, 1)
    neighbours = padded_red[:-2, 1:-1] + padded_red[2:, 1:-1] + padded_red[1:-1, :-2] + padded_red[1:-1, 2:]
    row_pos = jnp.arange(H, dtype=jnp.int32)
    col_pos = jnp.arange(W, dtype=jnp.int32)
    vertical_strip_bounds = (row_pos == 0).astype(jnp.float32) + (row_pos == H - 1).astype(jnp.float32)
    col_edges = (col_pos == 0).astype(jnp.float32) + (col_pos == W - 1).astype(jnp.float32)
    counted = 4.0 - vertical_strip_bounds[:, None] - col_edges[None, :]
    centre = 0.5 * upsampled + 0.5 * neighbours / counted
    black = estimate(chosen_hypothesis, candidate, centre)
    parity = (row_pos[:, None] + col_pos[None, :]) % 2 == 0
    return jnp.where(parity, red, black)
```

```python
import functools

import jax
import jax.numpy as jnp
from jax import lax
from jax.experimental import pallas as pl
from jax.experimental.pallas import tpu as pltpu
from jax.sharding import PartitionSpec as P

LEVELS = 16
HYP = 8
SRC = 4
MAXID = 3
WIN = 11
UPS = 8
CITER = 4
RAD = WIN // 2
LANES = 128
Q = 8
EDGE = 8
PADC = 8
LEFT = -(-(MAXID * (LEVELS - 1) + RAD) // 8) * 8
MLEFT = -(-(MAXID * (LEVELS - 1)) // 8) * 8

FLOOR = 1e-05
AREA = float(WIN * WIN)
F32 = jnp.float32
BF16 = jnp.bfloat16
MESH = pl.DeviceIdType.MESH


def col_box(p, n):
    s2 = p[: n + 9] + p[1 : n + 10]
    s4 = s2[: n + 7] + s2[2 : n + 9]
    s8 = s4[:n] + s4[4 : n + 4]
    return s8 + s2[8 : n + 8] + p[10 : n + 10]


def split3(y):
    y = y.reshape(-1, LANES)
    hi = y.astype(BF16)
    rest = y - hi.astype(F32)
    mid = rest.astype(BF16)
    low = (rest - mid.astype(F32)).astype(BF16)
    return hi, mid, low


def row_box(main, extra, weight):
    out = None
    for m, e in zip(main, extra):
        d = jnp.dot(jnp.concatenate([m, e], 1), weight, preferred_element_type=F32)
        out = d if out is None else out + d
    return out.reshape(-1, Q, LANES)


def interp_pair(fine, total):
    num = 2 * fine + (1 - UPS)
    shift = (2 * UPS).bit_length() - 1
    lower = lax.shift_right_arithmetic(num, jnp.full_like(num, shift))
    frac = (num - lower * (2 * UPS)).astype(F32) * (1.0 / (2 * UPS))
    lo = jnp.clip(lower, 0, total - 1)
    hi = jnp.clip(lower + 1, 0, total - 1)
    return lo, hi, frac


def iota(shape, dim):
    return lax.broadcasted_iota(jnp.int32, shape, dim)


def kernel(nr, nc, ids, ref, src, hyp, cd_ref, cc_ref, out, xt, up, down, corner, xe, ov, ove,
           mom, rmom, sel, cand, disp, conf, band, redt, redrow, edge, ups, work, send, recv):
    rows, cols = ref.shape
    tt = cols // Q
    r, c = lax.axis_index("row"), lax.axis_index("col")
    block = cd_ref.shape[0]
    ncr, ncc = block * nc, cd_ref.shape[1]
    ct = rows // UPS
    uu = LEFT + tt + EDGE
    ww = MLEFT + tt

    def peer(dr, dc):
        return {"row": lax.rem(r + dr + nr, nr), "col": lax.rem(c + dc + nc, nc)}

    offsets = sorted(
        {(dr % nr, dc % nc) for dr in (-1, 0, 1) for dc in (-1, 0, 1)}
        | {(0, dc) for dc in range(nc)}
    )
    offsets = [o for o in offsets if o != (0, 0)]
    barrier = pltpu.get_barrier_semaphore()
    for dr, dc in offsets:
        pl.semaphore_signal(barrier, inc=1, device_id=peer(dr, dc), device_id_type=MESH)

    zero_pad = jnp.zeros((PADC, ncc), F32)
    for grid_ref in (disp, conf):
        grid_ref[0:PADC] = zero_pad
        grid_ref[PADC + ncr : 2 * PADC + ncr] = zero_pad
    mine = pl.multiple_of(PADC + block * c, 8)
    disp[pl.ds(mine, block)] = cd_ref[...]
    conf[pl.ds(mine, block)] = cc_ref[...]
    pl.semaphore_wait(barrier, len(offsets))

    copies = []

    def push(a, b, dr, dc):
        k = len(copies)
        copy = pltpu.make_async_remote_copy(
            src_ref=a, dst_ref=b, send_sem=send.at[k], recv_sem=recv.at[k],
            device_id=peer(dr, dc), device_id_type=MESH,
        )
        copy.start()
        copies.append(copy)
        return copy

    last = rows - EDGE
    near = []
    for dr, lo, dst in ((-1, 0, down), (1, last, up)):
        near.append(push(ref.at[pl.ds(lo, EDGE)], dst.at[0], dr, 0))
        near.append(push(src.at[:, pl.ds(lo, EDGE)], dst.at[pl.ds(1, SRC)], dr, 0))
    for dr, lo, vert in ((-1, 0, 1), (1, last, 0)):
        for dc, cl, side in ((-1, 0, 1), (1, cols - LANES, 0)):
            dst = corner.at[vert, side]
            near.append(push(ref.at[pl.ds(lo, EDGE), pl.ds(cl, LANES)], dst.at[0], dr, dc))
            near.append(push(
                src.at[:, pl.ds(lo, EDGE), pl.ds(cl, LANES)], dst.at[pl.ds(1, SRC)], dr, dc
            ))
    for a in range(SRC + 1):
        image = ref[...] if a == 0 else src[a - 1]
        xt[a, LEFT : LEFT + cols] = image.T
    strips = [
        push(xt.at[:, pl.ds(cols, LEFT)], xt.at[:, pl.ds(0, LEFT)], 0, 1),
        push(xt.at[:, pl.ds(LEFT, EDGE)], xt.at[:, pl.ds(LEFT + cols, EDGE)], 0, -1),
    ]
    coarse = []
    for o in range(1, nc):
        for a, b in ((cd_ref, disp), (cc_ref, conf)):
            coarse.append(push(a, b.at[pl.ds(mine, block)], 0, o))

    def hyp_step(k, carry):
        work[...] = hyp[k].astype(F32).T
        for t in range(tt):
            cand[k, t] = work[pl.ds(t, Q, stride=tt), :]
        return carry

    lax.fori_loop(0, HYP, hyp_step, 0)

    kk = iota((2 * LANES, LANES), 0)
    oo = iota((2 * LANES, LANES), 1)
    for v in range(SRC):
        e = kk - LANES - 2 * EDGE * v
        pos = jnp.where(kk < LANES, kk, jnp.where(e < EDGE, e - EDGE, LANES + e - EDGE))
        ok = (jnp.abs(pos - oo) <= RAD) & ((kk < LANES) | ((e >= 0) & (e < 2 * EDGE)))
        band[v] = jnp.where(ok, 1.0, 0.0).astype(BF16)

    for copy in coarse:
        copy.wait()
    win = ct + 2 * PADC
    start = pl.multiple_of(ct * r, 8)
    d0 = disp[pl.ds(start, win)]
    f0 = conf[pl.ds(start, win)]
    grid_row = iota((win, ncc), 0) + (ct * r - PADC)
    valid = (grid_row >= 0) & (grid_row < ncr)
    lane = iota((win, ncc), 1)
    inv = jnp.where(valid, 1.0 / (f0 + 4.0), 0.0)
    base = f0 * d0
    cur = d0
    for _ in range(CITER):
        nb = pltpu.roll(cur, 1, 0) + pltpu.roll(cur, win - 1, 0)
        nb = nb + jnp.where(lane == 0, 0.0, pltpu.roll(cur, 1, 1))
        nb = nb + jnp.where(lane == ncc - 1, 0.0, pltpu.roll(cur, ncc - 1, 1))
        cur = (base + nb) * inv
    m = iota((cols, ncc), 0)
    lo, hi, frac = interp_pair(c * cols + lax.rem(m, Q) * tt + lax.div(m, Q), ncc)
    cl = iota((cols, ncc), 1)
    cmat = jnp.where(cl == lo, 1.0 - frac, 0.0) + jnp.where(cl == hi, frac, 0.0)
    lo, hi, frac = interp_pair(r * rows + iota((win, rows), 1), ncr)
    rl = iota((win, rows), 0) + (ct * r - PADC)
    rmat = jnp.where(rl == lo, 1.0 - frac, 0.0) + jnp.where(rl == hi, frac, 0.0)
    wide = lax.dot_general(
        cmat, cur, (((1,), (1,)), ((), ())), precision=lax.Precision.HIGHEST,
        preferred_element_type=F32,
    )
    ups[...] = jnp.dot(
        wide, rmat, precision=lax.Precision.HIGHEST, preferred_element_type=F32
    ).reshape(tt, Q, LANES)

    for copy in near:
        copy.wait()
    top, bottom, lside, rside = r > 0, r < nr - 1, c > 0, c < nc - 1

    def halo_rows(get_up, get_down, ok):
        for w in range(2):
            parts = []
            for v in range(SRC):
                a = 0 if w == 0 else v + 1
                parts.append(jnp.where(top & ok, get_up(a), 0.0))
                parts.append(jnp.where(bottom & ok, get_down(a), 0.0))
            parts.append(jnp.zeros((LANES - 2 * EDGE * SRC, LANES), F32))
            yield w, jnp.concatenate(parts, 0).T

    for b in range(cols // LANES):
        s = b * LANES
        for w, x in halo_rows(
            lambda a: up[a, :, s : s + LANES], lambda a: down[a, :, s : s + LANES], True
        ):
            xe[w, LEFT + s : LEFT + s + LANES] = x
    for w, x in halo_rows(lambda a: corner[0, 0, a], lambda a: corner[1, 0, a], lside):
        xe[w, 0:LEFT] = x[LANES - LEFT :]
    for w, x in halo_rows(lambda a: corner[0, 1, a], lambda a: corner[1, 1, a], rside):
        xe[w, LEFT + cols : LEFT + cols + EDGE] = x[:EDGE]
    for copy in strips:
        copy.wait()

    @pl.when(c == 0)
    def _():
        xt[:, 0:LEFT] = jnp.zeros((SRC + 1, LEFT, LANES), F32)

    @pl.when(c == nc - 1)
    def _():
        xt[:, LEFT + cols : LEFT + cols + EDGE] = jnp.zeros((SRC + 1, EDGE, LANES), F32)

    def spread(b, carry):
        for k in range(8):
            u = b * 8 + k
            for a in range(SRC + 1):
                ov[a, u] = xt[a, pl.ds(u, Q, stride=tt), :]
            for w in range(2):
                ove[w, u] = xe[w, pl.ds(u, Q, stride=tt), :]
        return carry

    lax.fori_loop(0, uu // 8, spread, 0)

    def mean_and_scale(x, e, n, v):
        means = row_box(split3(col_box(x, n)), e[0], band[v]) * (1.0 / AREA)
        squares = row_box(split3(col_box(x * x, n)), e[1], band[v]) * (1.0 / AREA)
        return means, lax.rsqrt(squares - means * means + FLOOR)

    mb = 16
    off = LEFT - RAD

    def ref_moments(b, carry):
        at = b * mb
        x = ov[0, pl.ds(off + at, mb + WIN - 1)]
        e = ove[0, pl.ds(off + at, mb + WIN - 1)]
        es = split3(col_box(e, mb)), split3(col_box(e * e, mb))
        mean, scale = mean_and_scale(x, es, mb, 0)
        rmom[0, pl.ds(at, mb)] = mean
        rmom[1, pl.ds(at, mb)] = scale * (1.0 / SRC)
        return carry

    lax.fori_loop(0, tt // mb, ref_moments, 0)

    def src_moments(b, carry):
        at = b * mb
        u = at + off - MLEFT
        e = ove[1, pl.ds(u, mb + WIN - 1)]
        es = split3(col_box(e, mb)), split3(col_box(e * e, mb))
        for v in range(SRC):
            x = ov[v + 1, pl.ds(u, mb + WIN - 1)]
            mean, scale = mean_and_scale(x, es, mb, v)
            mom[v, 0, pl.ds(at, mb)] = mean
            mom[v, 1, pl.ds(at, mb)] = scale
        return carry

    lax.fori_loop(0, ww // mb, src_moments, 0)

    sel[...] = jnp.zeros(sel.shape, F32)
    group = lax.shift_right_logical(iota((1, Q, LANES), 2), jnp.full((1, Q, LANES), 4))
    tb = 16
    span = tb + WIN - 1

    def level(i, carry):
        depth = lax.div(i, tt // tb)
        at = lax.rem(i, tt // tb) * tb
        moved = [ids[v] * depth for v in range(SRC)]
        e = ove[1, pl.ds(off + at - moved[0], span)]
        for v in range(1, SRC):
            e = jnp.where(group == v, ove[1, pl.ds(off + at - moved[v], span)], e)
        es = split3(col_box(e * ove[0, pl.ds(off + at, span)], tb))
        x0 = ov[0, pl.ds(off + at, span)]
        mr = rmom[0, pl.ds(at, tb)]
        total = None
        for v in range(SRC):
            y = col_box(x0 * ov[v + 1, pl.ds(off + at - moved[v], span)], tb)
            cross = row_box(split3(y), es, band[v]) * (1.0 / AREA)
            wi = MLEFT + at - moved[v]
            part = (cross - mr * mom[v, 0, pl.ds(wi, tb)]) * mom[v, 1, pl.ds(wi, tb)]
            total = part if total is None else total + part
        volume = total * rmom[1, pl.ds(at, tb)]
        depth_f = depth.astype(F32)
        for k in range(HYP):
            sel[k, pl.ds(at, tb)] = jnp.where(
                cand[k, pl.ds(at, tb)] == depth_f, volume, sel[k, pl.ds(at, tb)]
            )
        return carry

    lax.fori_loop(0, LEVELS * (tt // tb), level, 0)

    def estimate(at, n, centre):
        num = den = None
        for k in range(HYP):
            ck = cand[k, pl.ds(at, n)]
            diff = ck - centre
            wt = jnp.exp((sel[k, pl.ds(at, n)] - 1.0 - 0.01 * diff * diff) * 10.0)
            num = wt * ck if num is None else num + wt * ck
            den = wt if den is None else den + wt
        return num / den

    eb = 8

    def red_step(b, carry):
        at = b * eb
        red = estimate(at, eb, ups[pl.ds(at, eb)])
        for k in range(eb):
            redt[pl.ds(EDGE + at + k, Q, stride=tt), :] = red[k]
        return carry

    lax.fori_loop(0, tt // eb, red_step, 0)
    redrow[0] = redt[EDGE : EDGE + cols, :].T[0:EDGE]
    redrow[1] = redt[EDGE : EDGE + cols, :].T[last:rows]
    borders = [
        push(redt.at[pl.ds(EDGE, EDGE)], redt.at[pl.ds(EDGE + cols, EDGE)], 0, -1),
        push(redt.at[pl.ds(cols, EDGE)], redt.at[pl.ds(0, EDGE)], 0, 1),
        push(redrow.at[0], redrow.at[3], -1, 0),
        push(redrow.at[1], redrow.at[2], 1, 0),
    ]
    for copy in borders:
        copy.wait()
    row_no = iota((rows, cols), 0)
    above = jnp.where(top, redrow[2][EDGE - 1 : EDGE], 0.0)
    below = jnp.where(bottom, redrow[3][0:1], 0.0)
    edge[...] = jnp.where(row_no == 0, above, jnp.where(row_no == rows - 1, below, 0.0)).T

    @pl.when(c == 0)
    def _():
        redt[0:EDGE] = jnp.zeros((EDGE, LANES), F32)

    @pl.when(c == nc - 1)
    def _():
        redt[EDGE + cols : 2 * EDGE + cols] = jnp.zeros((EDGE, LANES), F32)

    lane2 = iota((Q, LANES), 1)
    chunk = iota((Q, LANES), 0)
    gi = r * rows + lane2
    rcount = 4.0 - jnp.where(gi == 0, 1.0, 0.0) - jnp.where(gi == nr * rows - 1, 1.0, 0.0)

    def black_step(t, carry):
        red = redt[pl.ds(EDGE + t, Q, stride=tt), :]
        nb = redt[pl.ds(EDGE - 1 + t, Q, stride=tt), :] + redt[pl.ds(EDGE + 1 + t, Q, stride=tt), :]
        nb = nb + jnp.where(lane2 == 0, 0.0, pltpu.roll(red, 1, 1))
        nb = nb + jnp.where(lane2 == LANES - 1, 0.0, pltpu.roll(red, LANES - 1, 1))
        nb = nb + edge[pl.ds(t, Q, stride=tt), :]
        gj = c * cols + chunk * tt + t
        count = rcount - jnp.where(gj == 0, 1.0, 0.0) - jnp.where(gj == nc * cols - 1, 1.0, 0.0)
        centre = 0.5 * ups[t] + 0.5 * nb / count
        black = estimate(t, 1, centre[None])[0]
        even = lax.rem(gi + gj, 2) == 0
        work[pl.ds(t, Q, stride=tt), :] = jnp.where(even, red, black)
        return carry

    lax.fori_loop(0, tt, black_step, 0)
    out[...] = work[...].T


def on_device(nr, nc, reference_image, source_images, hypotheses, source_ids, disp, conf):
    rows, cols = reference_image.shape
    tt = cols // Q
    block, ncc = disp.shape
    uu = LEFT + tt + EDGE
    ww = MLEFT + tt
    full = LEFT + cols + EDGE
    count = 4 + 8 + 2 + 2 * (nc - 1) + 4
    v = lambda *s: pltpu.VMEM(s, F32)
    vmem = pl.BlockSpec(memory_space=pltpu.VMEM)
    return pl.pallas_call(
        functools.partial(kernel, nr, nc),
        out_shape=jax.ShapeDtypeStruct((rows, cols), F32),
        in_specs=[pl.BlockSpec(memory_space=pltpu.SMEM)] + [vmem] * 5,
        out_specs=vmem,
        scratch_shapes=[
            v(SRC + 1, full, LANES),
            v(SRC + 1, EDGE, cols),
            v(SRC + 1, EDGE, cols),
            v(2, 2, SRC + 1, EDGE, LANES),
            v(2, full, LANES),
            v(SRC + 1, uu, Q, LANES),
            v(2, uu, Q, LANES),
            v(SRC, 2, ww, Q, LANES),
            v(2, tt, Q, LANES),
            v(HYP, tt, Q, LANES),
            v(HYP, tt, Q, LANES),
            v(block * nc + 2 * PADC, ncc),
            v(block * nc + 2 * PADC, ncc),
            pltpu.VMEM((SRC, 2 * LANES, LANES), BF16),
            v(cols + 2 * EDGE, LANES),
            v(4, EDGE, cols),
            v(cols, LANES),
            v(tt, Q, LANES),
            v(cols, LANES),
            pltpu.SemaphoreType.DMA((count,)),
            pltpu.SemaphoreType.DMA((count,)),
        ],
        compiler_params=pltpu.CompilerParams(
            collective_id=0, has_side_effects=True, vmem_limit_bytes=48 * 1024 * 1024
        ),
        name="stereo",
    )(source_ids, reference_image, source_images, hypotheses, disp, conf)


def solution(mesh):
    nr, nc = mesh.shape["row"], mesh.shape["col"]
    in_specs = (
        P("row", "col"),
        P(None, "row", "col"),
        P(None, "row", "col"),
        P(),
        P("col", None),
        P("col", None),
    )
    return jax.shard_map(
        functools.partial(on_device, nr, nc),
        mesh=mesh, in_specs=in_specs, out_specs=P("row", "col"), check_vma=False,
    )
```

```python
import functools

import jax
import jax.numpy as jnp
from jax import lax
from jax.experimental import pallas as pl
from jax.experimental.pallas import tpu as pltpu
from jax.sharding import PartitionSpec as P

LEVELS = 16
HYP = 8
SRC = 4
MAXID = 3
WIN = 11
UPS = 8
CITER = 4
RAD = WIN // 2
LANES = 128
Q = 8
EDGE = 8
PADC = 8
LEFT = -(-(MAXID * (LEVELS - 1) + RAD) // 8) * 8
MLEFT = -(-(MAXID * (LEVELS - 1)) // 8) * 8

FLOOR = 1e-05
AREA = float(WIN * WIN)
F32 = jnp.float32
BF16 = jnp.bfloat16
MESH = pl.DeviceIdType.MESH


def col_box(p, n):
    s2 = p[: n + 9] + p[1 : n + 10]
    s4 = s2[: n + 7] + s2[2 : n + 9]
    s8 = s4[:n] + s4[4 : n + 4]
    return s8 + s2[8 : n + 8] + p[10 : n + 10]


def split3(y):
    y = y.reshape(-1, LANES)
    hi = y.astype(BF16)
    rest = y - hi.astype(F32)
    mid = rest.astype(BF16)
    low = (rest - mid.astype(F32)).astype(BF16)
    return hi, mid, low


def row_box(main, extra, weight):
    pieces = [x for pair in zip(main, extra) for x in pair]
    out = jnp.dot(jnp.concatenate(pieces, 1), weight[...], preferred_element_type=F32)
    return out.reshape(-1, Q, LANES)


def interp_pair(fine, total):
    num = 2 * fine + (1 - UPS)
    shift = (2 * UPS).bit_length() - 1
    lower = lax.shift_right_arithmetic(num, jnp.full_like(num, shift))
    frac = (num - lower * (2 * UPS)).astype(F32) * (1.0 / (2 * UPS))
    lo = jnp.clip(lower, 0, total - 1)
    hi = jnp.clip(lower + 1, 0, total - 1)
    return lo, hi, frac


def iota(shape, dim):
    return lax.broadcasted_iota(jnp.int32, shape, dim)


def kernel(nr, nc, ids_h, ref_h, src_h, hyp_h, cd_ref, cc_ref, out, ids, ref, src, hyp, local, xt, up, down, corner, xe, ov, ove,
           mom, rmom, sel, cand, disp, conf, band, redt, redrow, edge, ups, work, send, recv):
    rows, cols = ref.shape
    tt = cols // Q
    r, c = lax.axis_index("row"), lax.axis_index("col")
    block = cd_ref.shape[0]
    ncr, ncc = block * nc, cd_ref.shape[1]
    ct = rows // UPS
    uu = LEFT + tt + EDGE
    ww = MLEFT + tt

    def peer(dr, dc):
        return {"row": lax.rem(r + dr + nr, nr), "col": lax.rem(c + dc + nc, nc)}

    offsets = sorted(
        {(dr % nr, dc % nc) for dr in (-1, 0, 1) for dc in (-1, 0, 1)}
        | {(0, dc) for dc in range(nc)}
    )
    offsets = [o for o in offsets if o != (0, 0)]
    barrier = pltpu.get_barrier_semaphore()
    for dr, dc in offsets:
        pl.semaphore_signal(barrier, inc=1, device_id=peer(dr, dc), device_id_type=MESH)

    mine = pl.multiple_of(PADC + block * c, 8)
    loads = []
    for a, b in ((ref_h, ref), (src_h, src), (cd_ref, disp.at[pl.ds(mine, block)]),
                 (cc_ref, conf.at[pl.ds(mine, block)]), (ids_h, ids), (hyp_h, hyp)):
        loads.append(pltpu.make_async_copy(a, b, local.at[len(loads)]))
        loads[-1].start()
    zero_pad = jnp.zeros((PADC, ncc), F32)
    for grid_ref in (disp, conf):
        grid_ref[0:PADC] = zero_pad
        grid_ref[PADC + ncr : 2 * PADC + ncr] = zero_pad
    pl.semaphore_wait(barrier, len(offsets))

    copies = []

    def push(a, b, dr, dc):
        k = len(copies)
        copy = pltpu.make_async_remote_copy(
            src_ref=a, dst_ref=b, send_sem=send.at[k], recv_sem=recv.at[k],
            device_id=peer(dr, dc), device_id_type=MESH,
        )
        copy.start()
        copies.append(copy)
        return copy

    last = rows - EDGE
    near = []
    for dr, lo, dst in ((-1, 0, down), (1, last, up)):
        near.append(push(ref_h.at[pl.ds(lo, EDGE)], dst.at[0], dr, 0))
        near.append(push(src_h.at[:, pl.ds(lo, EDGE)], dst.at[pl.ds(1, SRC)], dr, 0))
    for dr, lo, vert in ((-1, 0, 1), (1, last, 0)):
        for dc, cl, side in ((-1, 0, 1), (1, cols - LANES, 0)):
            dst = corner.at[vert, side]
            near.append(push(ref_h.at[pl.ds(lo, EDGE), pl.ds(cl, LANES)], dst.at[0], dr, dc))
            near.append(push(
                src_h.at[:, pl.ds(lo, EDGE), pl.ds(cl, LANES)], dst.at[pl.ds(1, SRC)], dr, dc
            ))
    coarse = []
    for o in range(1, nc):
        for a, b in ((cd_ref, disp), (cc_ref, conf)):
            coarse.append(push(a, b.at[pl.ds(mine, block)], 0, o))
    strips = []
    loads[0].wait()
    loads[1].wait()
    for a in range(1, SRC + 1):
        xt[a, LEFT : LEFT + cols] = src[a - 1].T
        strips.append(push(xt.at[a, pl.ds(cols, LEFT)], xt.at[a, pl.ds(0, LEFT)], 0, 1))
    xt[0, LEFT : LEFT + cols] = ref[...].T
    strips.append(push(
        xt.at[0, pl.ds(LEFT + cols - EDGE, EDGE)], xt.at[0, pl.ds(LEFT - EDGE, EDGE)], 0, 1
    ))
    strips.append(push(
        xt.at[:, pl.ds(LEFT, EDGE)], xt.at[:, pl.ds(LEFT + cols, EDGE)], 0, -1
    ))

    loads[5].wait()

    def hyp_step(k, carry):
        work[...] = hyp[k].astype(F32).T
        for t in range(tt):
            cand[k, t] = work[pl.ds(t, Q, stride=tt), :]
        return carry

    lax.fori_loop(0, HYP, hyp_step, 0)

    kk = iota((2 * LANES, LANES), 0)
    oo = iota((2 * LANES, LANES), 1)
    for v in range(SRC):
        e = kk - LANES - 2 * EDGE * v
        pos = jnp.where(kk < LANES, kk, jnp.where(e < EDGE, e - EDGE, LANES + e - EDGE))
        ok = (jnp.abs(pos - oo) <= RAD) & ((kk < LANES) | ((e >= 0) & (e < 2 * EDGE)))
        for i in range(3):
            band[v, 2 * LANES * i : 2 * LANES * (i + 1)] = jnp.where(ok, 1.0, 0.0).astype(BF16)

    def own_spread(b, carry):
        for k in range(8):
            u = LEFT + b * 8 + k
            for a in range(SRC + 1):
                ov[a, u] = xt[a, pl.ds(u, Q, stride=tt), :]
        return carry

    lax.fori_loop(0, tt // 8, own_spread, 0)

    for copy in coarse + loads[2:5]:
        copy.wait()
    win = ct + 2 * PADC
    start = pl.multiple_of(ct * r, 8)
    d0 = disp[pl.ds(start, win)]
    f0 = conf[pl.ds(start, win)]
    grid_row = iota((win, ncc), 0) + (ct * r - PADC)
    valid = (grid_row >= 0) & (grid_row < ncr)
    lane = iota((win, ncc), 1)
    inv = jnp.where(valid, 1.0 / (f0 + 4.0), 0.0)
    base = f0 * d0
    cur = d0
    for _ in range(CITER):
        nb = pltpu.roll(cur, 1, 0) + pltpu.roll(cur, win - 1, 0)
        nb = nb + jnp.where(lane == 0, 0.0, pltpu.roll(cur, 1, 1))
        nb = nb + jnp.where(lane == ncc - 1, 0.0, pltpu.roll(cur, ncc - 1, 1))
        cur = (base + nb) * inv
    m = iota((cols, ncc), 0)
    lo, hi, frac = interp_pair(c * cols + lax.rem(m, Q) * tt + lax.div(m, Q), ncc)
    cl = iota((cols, ncc), 1)
    cmat = jnp.where(cl == lo, 1.0 - frac, 0.0) + jnp.where(cl == hi, frac, 0.0)
    lo, hi, frac = interp_pair(r * rows + iota((win, rows), 1), ncr)
    rl = iota((win, rows), 0) + (ct * r - PADC)
    rmat = jnp.where(rl == lo, 1.0 - frac, 0.0) + jnp.where(rl == hi, frac, 0.0)
    wide = lax.dot_general(
        cmat, cur, (((1,), (1,)), ((), ())), precision=lax.Precision.HIGHEST,
        preferred_element_type=F32,
    )
    ups[...] = jnp.dot(
        wide, rmat, precision=lax.Precision.HIGHEST, preferred_element_type=F32
    ).reshape(tt, Q, LANES)

    for copy in near:
        copy.wait()
    top, bottom, lside, rside = r > 0, r < nr - 1, c > 0, c < nc - 1

    def halo_rows(get_up, get_down, ok):
        for w in range(2):
            parts = []
            for v in range(SRC):
                a = 0 if w == 0 else v + 1
                parts.append(jnp.where(top & ok, get_up(a), 0.0))
                parts.append(jnp.where(bottom & ok, get_down(a), 0.0))
            parts.append(jnp.zeros((LANES - 2 * EDGE * SRC, LANES), F32))
            yield w, jnp.concatenate(parts, 0).T

    for b in range(cols // LANES):
        s = b * LANES
        for w, x in halo_rows(
            lambda a: up[a, :, s : s + LANES], lambda a: down[a, :, s : s + LANES], True
        ):
            xe[w, LEFT + s : LEFT + s + LANES] = x
    for w, x in halo_rows(lambda a: corner[0, 0, a], lambda a: corner[1, 0, a], lside):
        xe[w, 0:LEFT] = x[LANES - LEFT :]
    for w, x in halo_rows(lambda a: corner[0, 1, a], lambda a: corner[1, 1, a], rside):
        xe[w, LEFT + cols : LEFT + cols + EDGE] = x[:EDGE]
    def spread(b, carry):
        for k in range(8):
            u = b * 8 + k
            for w in range(2):
                ove[w, u] = xe[w, pl.ds(u, Q, stride=tt), :]
        return carry

    lax.fori_loop(0, uu // 8, spread, 0)
    for copy in strips:
        copy.wait()

    @pl.when(c == 0)
    def _():
        xt[1:, 0:LEFT] = jnp.zeros((SRC, LEFT, LANES), F32)
        xt[0, LEFT - EDGE : LEFT] = jnp.zeros((EDGE, LANES), F32)

    @pl.when(c == nc - 1)
    def _():
        xt[:, LEFT + cols : LEFT + cols + EDGE] = jnp.zeros((SRC + 1, EDGE, LANES), F32)

    def halo_spread(b, carry):
        for k in range(8):
            u = lax.rem(b * 8 + LEFT + tt, uu) + k
            for a in range(1, SRC + 1):
                ov[a, u] = xt[a, pl.ds(u, Q, stride=tt), :]
        return carry

    lax.fori_loop(0, (uu - tt) // 8, halo_spread, 0)
    for k in range(EDGE):
        for u in (LEFT - EDGE + k, LEFT + tt + k):
            ov[0, u] = xt[0, pl.ds(u, Q, stride=tt), :]

    def mean_and_scale(x, e, n, v):
        means = row_box(split3(col_box(x, n)), e[0], band.at[v]) * (1.0 / AREA)
        squares = row_box(split3(col_box(x * x, n)), e[1], band.at[v]) * (1.0 / AREA)
        return means, lax.rsqrt(squares - means * means + FLOOR)

    mb = 16
    off = LEFT - RAD

    def ref_moments(b, carry):
        at = b * mb
        x = ov[0, pl.ds(off + at, mb + WIN - 1)]
        e = ove[0, pl.ds(off + at, mb + WIN - 1)]
        es = split3(col_box(e, mb)), split3(col_box(e * e, mb))
        mean, scale = mean_and_scale(x, es, mb, 0)
        rmom[0, pl.ds(at, mb)] = mean * AREA
        rmom[1, pl.ds(at, mb)] = scale * (1.0 / SRC)
        return carry

    lax.fori_loop(0, tt // mb, ref_moments, 0)

    mb2 = ww // 2
    def src_moments(b, carry):
        at = b * mb2
        u = at + off - MLEFT
        e = ove[1, pl.ds(u, mb2 + WIN - 1)]
        es = split3(col_box(e, mb2)), split3(col_box(e * e, mb2))
        for v in range(SRC):
            x = ov[v + 1, pl.ds(u, mb2 + WIN - 1)]
            mean, scale = mean_and_scale(x, es, mb2, v)
            mom[v, 0, pl.ds(at, mb2)] = mean
            mom[v, 1, pl.ds(at, mb2)] = scale * (1.0 / AREA)
        return carry

    lax.fori_loop(0, ww // mb2, src_moments, 0)

    sel[...] = jnp.zeros(sel.shape, F32)
    group = lax.shift_right_logical(iota((1, Q, LANES), 2), jnp.full((1, Q, LANES), 4))
    tb = 32
    span = tb + WIN - 1

    def level(i, carry):
        depth = lax.div(i, tt // tb)
        at = lax.rem(i, tt // tb) * tb
        moved = [ids[v] * depth for v in range(SRC)]
        e = ove[1, pl.ds(off + at - moved[0], span)]
        for v in range(1, SRC):
            e = jnp.where(group == v, ove[1, pl.ds(off + at - moved[v], span)], e)
        es = split3(col_box(e * ove[0, pl.ds(off + at, span)], tb))
        x0 = ov[0, pl.ds(off + at, span)]
        mr = rmom[0, pl.ds(at, tb)]
        total = None
        for v in range(SRC):
            y = col_box(x0 * ov[v + 1, pl.ds(off + at - moved[v], span)], tb)
            cross = row_box(split3(y), es, band.at[v])
            wi = MLEFT + at - moved[v]
            part = (cross - mr * mom[v, 0, pl.ds(wi, tb)]) * mom[v, 1, pl.ds(wi, tb)]
            total = part if total is None else total + part
        volume = total * rmom[1, pl.ds(at, tb)]
        depth_f = depth.astype(F32)
        for k in range(HYP):
            sel[k, pl.ds(at, tb)] = jnp.where(
                cand[k, pl.ds(at, tb)] == depth_f, volume, sel[k, pl.ds(at, tb)]
            )
        return carry

    lax.fori_loop(0, LEVELS * (tt // tb), level, 0)

    def estimate(at, n, centre):
        num = den = None
        for k in range(HYP):
            ck = cand[k, pl.ds(at, n)]
            diff = ck - centre
            wt = jnp.exp((sel[k, pl.ds(at, n)] - 1.0 - 0.01 * diff * diff) * 10.0)
            num = wt * ck if num is None else num + wt * ck
            den = wt if den is None else den + wt
        return num / den

    eb = 8

    def red_step(b, carry):
        at = b * eb
        red = estimate(at, eb, ups[pl.ds(at, eb)])
        for k in range(eb):
            redt[pl.ds(EDGE + at + k, Q, stride=tt), :] = red[k]
        return carry

    lax.fori_loop(0, tt // eb, red_step, 0)
    redrow[0] = redt[EDGE : EDGE + cols, :].T[0:EDGE]
    redrow[1] = redt[EDGE : EDGE + cols, :].T[last:rows]
    borders = [
        push(redt.at[pl.ds(EDGE, EDGE)], redt.at[pl.ds(EDGE + cols, EDGE)], 0, -1),
        push(redt.at[pl.ds(cols, EDGE)], redt.at[pl.ds(0, EDGE)], 0, 1),
        push(redrow.at[0], redrow.at[3], -1, 0),
        push(redrow.at[1], redrow.at[2], 1, 0),
    ]
    for copy in borders:
        copy.wait()
    row_no = iota((rows, cols), 0)
    above = jnp.where(top, redrow[2][EDGE - 1 : EDGE], 0.0)
    below = jnp.where(bottom, redrow[3][0:1], 0.0)
    edge[...] = jnp.where(row_no == 0, above, jnp.where(row_no == rows - 1, below, 0.0)).T

    @pl.when(c == 0)
    def _():
        redt[0:EDGE] = jnp.zeros((EDGE, LANES), F32)

    @pl.when(c == nc - 1)
    def _():
        redt[EDGE + cols : 2 * EDGE + cols] = jnp.zeros((EDGE, LANES), F32)

    lane2 = iota((Q, LANES), 1)
    chunk = iota((Q, LANES), 0)
    gi = r * rows + lane2
    rcount = 4.0 - jnp.where(gi == 0, 1.0, 0.0) - jnp.where(gi == nr * rows - 1, 1.0, 0.0)

    def black_step(b, carry):
        for t in [b * bb + k for k in range(bb)]:
            red = redt[pl.ds(EDGE + t, Q, stride=tt), :]
            nb = redt[pl.ds(EDGE - 1 + t, Q, stride=tt), :]
            nb = nb + redt[pl.ds(EDGE + 1 + t, Q, stride=tt), :]
            nb = nb + jnp.where(lane2 == 0, 0.0, pltpu.roll(red, 1, 1))
            nb = nb + jnp.where(lane2 == LANES - 1, 0.0, pltpu.roll(red, LANES - 1, 1))
            nb = nb + edge[pl.ds(t, Q, stride=tt), :]
            gj = c * cols + chunk * tt + t
            count = rcount - jnp.where(gj == 0, 1.0, 0.0)
            count = count - jnp.where(gj == nc * cols - 1, 1.0, 0.0)
            centre = 0.5 * ups[t] + 0.5 * nb / count
            black = estimate(t, 1, centre[None])[0]
            even = lax.rem(gi + gj, 2) == 0
            work[pl.ds(t, Q, stride=tt), :] = jnp.where(even, red, black)
        return carry

    bb = 4
    lax.fori_loop(0, tt // bb, black_step, 0)
    out[...] = work[...].T


def on_device(nr, nc, reference_image, source_images, hypotheses, source_ids, disp, conf):
    rows, cols = reference_image.shape
    tt = cols // Q
    block, ncc = disp.shape
    uu = LEFT + tt + EDGE
    ww = MLEFT + tt
    full = LEFT + cols + EDGE
    count = 4 + 8 + 6 + 2 * (nc - 1) + 4
    v = lambda *s: pltpu.VMEM(s, F32)
    vmem = pl.BlockSpec(memory_space=pltpu.VMEM)
    return pl.pallas_call(
        functools.partial(kernel, nr, nc),
        out_shape=jax.ShapeDtypeStruct((rows, cols), F32),
        in_specs=[pl.BlockSpec(memory_space=pl.ANY)] * 6,
        out_specs=vmem,
        scratch_shapes=[
            pltpu.SMEM((SRC,), jnp.int32),
            v(rows, cols),
            v(SRC, rows, cols),
            pltpu.VMEM((HYP, rows, cols), jnp.int32),
            pltpu.SemaphoreType.DMA((6,)),
            v(SRC + 1, full, LANES),
            v(SRC + 1, EDGE, cols),
            v(SRC + 1, EDGE, cols),
            v(2, 2, SRC + 1, EDGE, LANES),
            v(2, full, LANES),
            v(SRC + 1, uu, Q, LANES),
            v(2, uu, Q, LANES),
            v(SRC, 2, ww, Q, LANES),
            v(2, tt, Q, LANES),
            v(HYP, tt, Q, LANES),
            v(HYP, tt, Q, LANES),
            v(block * nc + 2 * PADC, ncc),
            v(block * nc + 2 * PADC, ncc),
            pltpu.VMEM((SRC, 6 * LANES, LANES), BF16),
            v(cols + 2 * EDGE, LANES),
            v(4, EDGE, cols),
            v(cols, LANES),
            v(tt, Q, LANES),
            v(cols, LANES),
            pltpu.SemaphoreType.DMA((count,)),
            pltpu.SemaphoreType.DMA((count,)),
        ],
        compiler_params=pltpu.CompilerParams(
            collective_id=0, has_side_effects=True, vmem_limit_bytes=60 * 1024 * 1024
        ),
        name="stereo",
    )(source_ids, reference_image, source_images, hypotheses, disp, conf)


def solution(mesh):
    nr, nc = mesh.shape["row"], mesh.shape["col"]
    in_specs = (
        P("row", "col"),
        P(None, "row", "col"),
        P(None, "row", "col"),
        P(),
        P("col", None),
        P("col", None),
    )
    return jax.shard_map(
        functools.partial(on_device, nr, nc),
        mesh=mesh, in_specs=in_specs, out_specs=P("row", "col"), check_vma=False,
    )
```
